256 devices in a mesh: sub: 64 (over z, y, core), grp: 4 (over x).
Axes of the slice: x: 4, y: 4, z: 8, core: 2. Of those that a mesh axis runs over, the one named last changes fastest.
Arguments:
- interior_factor: bfloat16 [256, 2048, 2048], P(('sub', 'grp')), may hold values from -0.25 to 2, as said below
- interface_coupling: bfloat16 [256, 2048, 512], P(('sub', 'grp')), may hold values from -0.09375 to 0.09375
- interface_block: float32 [256, 512, 512], P(('sub', 'grp')), may hold values from -0.5 to 4, as said below
- sample_panel: bfloat16 [32768, 128], P('sub'), may hold values from -6 to 6
- index_map: int32 [256, 4], P(('sub', 'grp')), may hold values from 0 to 255, as said below
- block_count: int32 [256], P(('sub', 'grp')), may hold values from 1 to 4
Outputs:
- sampled: float32 [32768, 128], P(('sub', 'grp'))
The draws below stay inside these ranges and needn't reach their ends.
Inputs may be any that keep to these rules, and one draw needn't show every extreme that they name: `index_map`: local block a of subdomain s is global block o * 4 + a, where o is s // 4, or one more or one less than it modulo 256 // 4. `interior_factor`: each matrix is lower triangular with its diagonal in 1 to 2. `interface_block`: each matrix is symmetric with its diagonal in 2 to 4.
All inputs are finite; a program needn't handle non-finite values.
Results may differ from the reference program's by a relative error of at most 0.0012.
Values sent between devices are 32-bit elements; how exact they have to be, the bound alone decides.
A program may use at most 64 MiB of HBM per device.

```python
import jax
import jax.numpy as jnp
from jax import lax

NI = 2048
NB = 512
BLK = 128
NS = 128
POWER = 3
LB = 4
NSUBD = 256
NG = 32768


def draw_interior_factor(key, part):

    def one_factor(sub_key):
        first, second = jax.random.split(sub_key)
        diagonal = jax.random.uniform(first, (NI,), jnp.float32, 1.0, 2.0)
        lower = jax.random.normal(second, (NI, NI), jnp.float32) * NI ** (-0.5)
        lower = jnp.clip(lower, -0.25, 0.25)
        matrix = jnp.tril(lower, -1) + jnp.diag(diagonal)
        return matrix.astype(jnp.bfloat16)
    return lax.map(one_factor, jax.random.split(key, NSUBD))


def draw_interface_block(key, part):

    def one_block(sub_key):
        first, second = jax.random.split(sub_key)
        diagonal = jax.random.uniform(first, (NB,), jnp.float32, 2.0, 4.0)
        noise = jax.random.normal(second, (NB, NB), jnp.float32) * 0.05
        symmetric = (noise + noise.T) * 0.7071
        symmetric = symmetric - jnp.diag(jnp.diag(symmetric))
        return symmetric + jnp.diag(diagonal)
    return lax.map(one_block, jax.random.split(key, NSUBD))


def draw_index_map(key, part):
    offsets = jax.random.randint(jax.random.fold_in(key, 7), (NSUBD, LB), -1, 2)
    cycles = NSUBD // LB
    home = jnp.arange(NSUBD, dtype=jnp.int32) // LB
    owner = (home[:, None] + offsets + cycles) % cycles
    return (owner * LB + jnp.arange(LB, dtype=jnp.int32)[None, :]).astype(jnp.int32)


def touch_ends(result, stream_key, least, top_value):
    spot = [jax.random.randint(jax.random.fold_in(stream_key, axis), (), 0, length) for axis, length in enumerate(result.shape)]
    longest = result.shape.index(max(result.shape))
    beside = spot[:longest] + [(spot[longest] + 1) % result.shape[longest]] + spot[longest + 1:]
    return result.at[tuple(spot)].set(least).at[tuple(beside)].set(top_value)


def level_of(stream_key, shape, cuts, low, largest):
    level, own = 1.0, jax.random.fold_in(stream_key, 6)
    for position, parts in cuts:
        heights = jnp.exp(jax.random.uniform(jax.random.fold_in(own, position), (parts,), jnp.float32, low / len(cuts), largest / len(cuts)))
        level = level * jnp.repeat(heights, shape[position] // parts).reshape([-1 if axis == position else 1 for axis in range(len(shape))])
    return level


def centred(rng, dims, deviation, limit, cuts=(), held_as=jnp.bfloat16):
    values = jax.random.normal(rng, dims, jnp.float32) * deviation
    if len(cuts) > 0:
        values = level_of(rng, dims, cuts, -0.22, 0.18) * values
    return jnp.clip(values, min=-limit, max=limit).astype(held_as)


def setup_inputs(seed: int = 0) -> dict:
    key_of = jax.random.split(jax.random.key(seed), 7)
    return {
        "interior_factor": draw_interior_factor(jax.random.fold_in(key_of[6], 71), 0),
        "interface_coupling": centred(key_of[1], (NSUBD, NI, NB), (2 * NI) ** -0.5, 0.09375, ((0, 256),)),
        "interface_block": draw_interface_block(jax.random.fold_in(key_of[6], 71), 0),
        "sample_panel": centred(key_of[3], (NG, NS), 1.0, 6.0, ((0, 64),)),
        "index_map": draw_index_map(jax.random.fold_in(key_of[6], 71), 0),
        "block_count": touch_ends(jax.random.randint(key_of[5], (NSUBD,), 1, LB + 1), jax.random.fold_in(key_of[5], 1), 1, LB).astype(jnp.int32),
    }


def form_schur(items):
    factor, coupling, block, count = items
    coupled = jnp.dot(factor, coupling, preferred_element_type=jnp.float32).astype(jnp.bfloat16)
    schur = block - jnp.dot(coupled.T, coupled, preferred_element_type=jnp.float32)
    live = (jnp.arange(LB, dtype=jnp.int32) < count).astype(jnp.float32)
    masked = schur.reshape(LB, BLK, LB, BLK) * live[:, None, None, None] * live[None, None, :, None]
    return masked.reshape(NB, NB)


def apply_fn(vector_blocks):
    def apply_one(items):
        masked, ids = items
        picked = vector_blocks[ids]
        product = jnp.dot(masked, picked.reshape(NB, NS), precision=lax.Precision.HIGHEST)
        return product.reshape(LB, BLK, NS)
    return apply_one


def reference(interior_factor, interface_coupling, interface_block, sample_panel, index_map, block_count):
    schurs = lax.map(form_schur, (interior_factor, interface_coupling, interface_block, block_count))
    vector_blocks = sample_panel.astype(jnp.float32).reshape(NSUBD, BLK, NS)
    for step in range(POWER):
        terms = lax.map(apply_fn(vector_blocks), (schurs, index_map))
        total = jnp.zeros((NSUBD, BLK, NS), jnp.float32)
        total = total.at[index_map.reshape(-1)].add(terms.reshape(NSUBD * LB, BLK, NS))
        vector_blocks = 0.5 * total
    return vector_blocks.reshape(NG, NS)
```

```python
import functools

import jax
import jax.numpy as jnp
from jax import lax
from jax.experimental import pallas as pl
from jax.experimental.pallas import tpu as pltpu
from jax.sharding import PartitionSpec as P

POWER = 3
CHUNKS = 2
MESH = pl.DeviceIdType.MESH


def halves(x):
    hi = x.astype(jnp.bfloat16)
    lo = (x - hi.astype(jnp.float32)).astype(jnp.bfloat16)
    return hi, lo


def body(
    cycles,
    groups,
    factor_hbm,
    coupling_hbm,
    block_hbm,
    panel_hbm,
    ids_hbm,
    count_hbm,
    out_ref,
    factor,
    coupling,
    block,
    panel,
    ids,
    count,
    coupled,
    m_hi,
    m_lo,
    halo,
    idx_mine,
    idx_far,
    p_mine,
    p_far,
    t_mine,
    near_low,
    near_high,
    far_low,
    far_high,
    v_mine,
    x_all,
    v_last,
    in_sems,
    halo_send,
    halo_recv,
    idx_send,
    idx_recv,
    p_send,
    p_recv,
    t_send,
    t_recv,
    v_send,
    v_recv,
):
    home = lax.axis_index("sub")
    mine = lax.axis_index("grp")
    size = factor.shape[0]
    width = block.shape[0]
    blk = width // groups
    samples = panel.shape[1]
    part = samples // CHUNKS
    rows = min(256, size)
    tiles = size // rows

    def ring(step):
        return lax.rem(home + step + cycles, cycles)

    def member(step):
        return lax.rem(mine + step, groups)

    loads = [
        pltpu.make_async_copy(ids_hbm, ids, in_sems.at[0]),
        pltpu.make_async_copy(count_hbm, count, in_sems.at[1]),
        pltpu.make_async_copy(panel_hbm, panel, in_sems.at[2]),
    ]
    for load in loads:
        load.start()
    factor_loads, coupling_loads = [], []
    for i in range(tiles):
        span = pl.ds(i * rows, rows)
        edge = pl.ds(0, (i + 1) * rows)
        coupling_loads.append(
            pltpu.make_async_copy(
                coupling_hbm.at[span, :], coupling.at[span, :], in_sems.at[4 + 2 * i]
            )
        )
        factor_loads.append(
            pltpu.make_async_copy(
                factor_hbm.at[span, edge], factor.at[span, edge], in_sems.at[5 + 2 * i]
            )
        )
        coupling_loads[i].start()
        factor_loads[i].start()
    block_load = pltpu.make_async_copy(block_hbm, block, in_sems.at[3])
    block_load.start()

    barrier = pltpu.get_barrier_semaphore()
    partners = [(ring(s), mine) for s in (-2, -1, 1, 2)]
    partners += [(home, member(r)) for r in range(1, groups)]
    for partner in partners:
        pl.semaphore_signal(barrier, inc=1, device_id=partner, device_id_type=MESH)

    for load in loads:
        load.wait()
    for b in range(groups):
        rows_b = panel[b * blk : (b + 1) * blk, :].astype(jnp.float32).T
        for c in range(CHUNKS):
            halo[c, 1, b] = rows_b[c * part : (c + 1) * part, :]
    for a in range(groups):
        owner = ids[0, a] // groups
        away = lax.rem(owner - home + cycles + 1, cycles) - 1
        idx_mine[a] = jnp.full((8, 128), away, jnp.int32)

    def couple(i):
        coupling_loads[i].wait()
        factor_loads[i].wait()
        span = slice(i * rows, (i + 1) * rows)
        coupled[span, :] = jnp.dot(
            factor[span, : (i + 1) * rows],
            coupling[: (i + 1) * rows, :],
            preferred_element_type=jnp.float32,
        ).astype(jnp.bfloat16)

    early = min(3, tiles)
    for i in range(early):
        couple(i)

    pl.semaphore_wait(barrier, len(partners))
    sent = []

    def send(src, dst, send_sem, recv_sem, device):
        copy = pltpu.make_async_remote_copy(
            src_ref=src,
            dst_ref=dst,
            send_sem=send_sem,
            recv_sem=recv_sem,
            device_id=device,
            device_id_type=MESH,
        )
        copy.start()
        sent.append(copy)
        return copy

    idx_copies = []
    for r in range(1, groups):
        idx_copies.append(
            send(
                idx_mine.at[member(r)],
                idx_far.at[r - 1],
                idx_send.at[r - 1],
                idx_recv.at[r - 1],
                (home, member(r)),
            )
        )
    halo_copies = []
    for c in range(CHUNKS):
        up = send(
            halo.at[c, 1], halo.at[c, 0], halo_send.at[c, 0], halo_recv.at[c, 0], (ring(1), mine)
        )
        down = send(
            halo.at[c, 1], halo.at[c, 2], halo_send.at[c, 1], halo_recv.at[c, 1], (ring(-1), mine)
        )
        halo_copies.append((up, down))

    for i in range(early, tiles):
        couple(i)

    block_load.wait()
    live = count[0]
    for a in range(groups):
        span = slice(a * blk, (a + 1) * blk)
        gram = lax.dot_general(
            coupled[:, span],
            coupled[...],
            (((0,), (0,)), ((), ())),
            preferred_element_type=jnp.float32,
        )
        schur = block[span, :] - gram
        column = lax.broadcasted_iota(jnp.int32, (blk, width), 1) // blk
        limit = jnp.where(a < live, live, 0)
        schur = jnp.where(column < limit, schur, 0.0)
        hi, lo = halves(schur)
        m_hi[span, :] = hi
        m_lo[span, :] = lo

    def pick(index, low, mid, high):
        index = index[None]
        return jnp.where(index == 0, mid, jnp.where(index < 0, low, high))

    def tiled(x):
        return x.reshape(x.shape[0] // 8, 8, x.shape[1])

    def flat(x):
        return x.reshape(x.shape[0] * 8, x.shape[2])

    def apply(x):
        hi, lo = halves(x)
        both = jnp.concatenate([hi, lo], axis=0)
        top = jnp.dot(both, m_hi[...], preferred_element_type=jnp.float32)
        low = jnp.dot(hi, m_lo[...], preferred_element_type=jnp.float32)
        return top[:part] + (top[part:] + low)

    def spread(t, c, x):
        product = apply(x)
        copies = []
        for a in range(groups):
            p_mine[t, c, a] = product[:, a * blk : (a + 1) * blk]
        for r in (2, 1, 3):
            copies.append(
                send(
                    p_mine.at[t, c, member(r)],
                    p_far.at[t, c, r - 1],
                    p_send.at[t, c, r - 1],
                    p_recv.at[t, c, r - 1],
                    (home, member(r)),
                )
            )
        return copies

    def first_x(c):
        up, down = halo_copies[c]
        up.wait_recv()
        down.wait_recv()
        pieces = []
        for b in range(groups):
            x = pick(
                idx_mine[b], tiled(halo[c, 0, b]), tiled(halo[c, 1, b]), tiled(halo[c, 2, b])
            )
            pieces.append(flat(x))
        return jnp.concatenate(pieces, axis=1)

    def next_x(t, c):
        return jnp.concatenate([x_all[t, c, b] for b in range(groups)], axis=1)

    def totals(t, c, copies):
        terms = [tiled(p_mine[t, c, mine])]
        where = [idx_mine[mine]]
        for copy in copies:
            copy.wait_recv()
        for r in range(1, groups):
            terms.append(tiled(p_far[t, c, r - 1]))
            where.append(idx_far[r - 1])
        out = []
        for e in (-1, 0, 1):
            total = None
            for term, index in zip(terms, where):
                kept = jnp.where(index[None] == e, term, 0.0)
                total = kept if total is None else total + kept
            out.append(flat(total))
        return out

    def pass_on(t, c, copies):
        low, mid, high = totals(t, c, copies)
        t_mine[t, c, 0] = low
        t_mine[t, c, 1] = mid
        t_mine[t, c, 2] = high
        if t == POWER - 1:
            return [
                send(
                    t_mine.at[t, c, 2],
                    near_low.at[t, c, 0],
                    t_send.at[t, c, 0],
                    t_recv.at[t, c, 0],
                    (ring(1), mine),
                ),
                send(
                    t_mine.at[t, c, 0],
                    near_high.at[t, c, 0],
                    t_send.at[t, c, 1],
                    t_recv.at[t, c, 1],
                    (ring(-1), mine),
                ),
            ]
        return [
            send(
                t_mine.at[t, c, pl.ds(1, 2)],
                near_low.at[t, c],
                t_send.at[t, c, 0],
                t_recv.at[t, c, 0],
                (ring(1), mine),
            ),
            send(
                t_mine.at[t, c, pl.ds(0, 2)],
                near_high.at[t, c],
                t_send.at[t, c, 1],
                t_recv.at[t, c, 1],
                (ring(-1), mine),
            ),
            send(
                t_mine.at[t, c, 2],
                far_low.at[t, c],
                t_send.at[t, c, 2],
                t_recv.at[t, c, 2],
                (ring(2), mine),
            ),
            send(
                t_mine.at[t, c, 0],
                far_high.at[t, c],
                t_send.at[t, c, 3],
                t_recv.at[t, c, 3],
                (ring(-2), mine),
            ),
        ]

    def choose(t, c, copies):
        for copy in copies:
            copy.wait_recv()
        low = tiled(0.5 * (t_mine[t, c, 0] + near_low[t, c, 0] + far_low[t, c]))
        mid = tiled(0.5 * (t_mine[t, c, 1] + near_low[t, c, 1] + near_high[t, c, 0]))
        high = tiled(0.5 * (t_mine[t, c, 2] + near_high[t, c, 1] + far_high[t, c]))
        out = []
        for r in (2, 1, 3):
            v_mine[t, c, r - 1] = flat(pick(idx_far[groups - r - 1], low, mid, high))
            out.append(
                send(
                    v_mine.at[t, c, r - 1],
                    x_all.at[t + 1, c, mine],
                    v_send.at[t, c, r - 1],
                    v_recv.at[t, c, r - 1],
                    (home, member(r)),
                )
            )
        x_all[t + 1, c, mine] = flat(pick(idx_mine[mine], low, mid, high))
        return out

    chunks = range(CHUNKS)
    moving = [spread(0, c, first_x(c)) for c in chunks]
    for copy in idx_copies:
        copy.wait_recv()
    for t in range(POWER):
        moving = [pass_on(t, c, moving[c]) for c in chunks]
        if t == POWER - 1:
            break
        moving = [choose(t, c, moving[c]) for c in chunks]
        following = []
        for c in chunks:
            for copy in moving[c]:
                copy.wait_recv()
            following.append(spread(t + 1, c, next_x(t + 1, c)))
        moving = following
    last = POWER - 1
    for c in chunks:
        for copy in moving[c]:
            copy.wait_recv()
        v_last[c * part : (c + 1) * part, :] = (
            t_mine[last, c, 1] + near_low[last, c, 0] + near_high[last, c, 0]
        )
    out_ref[...] = 0.5 * v_last[...].T
    for copy in sent:
        copy.wait_send()


def local(
    interior_factor, interface_coupling, interface_block, sample_panel, index_map, block_count
):
    cycles = lax.axis_size("sub")
    groups = lax.axis_size("grp")
    size = interior_factor.shape[1]
    width = interface_block.shape[1]
    blk = width // groups
    samples = sample_panel.shape[1]
    part = samples // CHUNKS
    f32, bf16 = jnp.float32, jnp.bfloat16
    dma = pltpu.SemaphoreType.DMA
    tiles = size // min(256, size)

    def vmem(*shape, dtype=f32):
        return pltpu.VMEM(shape, dtype)

    scratch = [
        vmem(size, size, dtype=bf16),
        vmem(size, width, dtype=bf16),
        vmem(width, width),
        vmem(width, samples, dtype=bf16),
        pltpu.SMEM((1, groups), jnp.int32),
        pltpu.SMEM((1,), jnp.int32),
        vmem(size, width, dtype=bf16),
        vmem(width, width, dtype=bf16),
        vmem(width, width, dtype=bf16),
        vmem(CHUNKS, 3, groups, part, blk),
        vmem(groups, 8, 128, dtype=jnp.int32),
        vmem(groups - 1, 8, 128, dtype=jnp.int32),
        vmem(POWER, CHUNKS, groups, part, blk),
        vmem(POWER, CHUNKS, groups - 1, part, blk),
        vmem(POWER, CHUNKS, 3, part, blk),
        vmem(POWER, CHUNKS, 2, part, blk),
        vmem(POWER, CHUNKS, 2, part, blk),
        vmem(POWER, CHUNKS, part, blk),
        vmem(POWER, CHUNKS, part, blk),
        vmem(POWER, CHUNKS, groups - 1, part, blk),
        vmem(POWER, CHUNKS, groups, part, blk),
        vmem(samples, blk),
        dma((4 + 2 * tiles,)),
        dma((CHUNKS, 2)),
        dma((CHUNKS, 2)),
        dma((groups - 1,)),
        dma((groups - 1,)),
        dma((POWER, CHUNKS, groups - 1)),
        dma((POWER, CHUNKS, groups - 1)),
        dma((POWER, CHUNKS, 4)),
        dma((POWER, CHUNKS, 4)),
        dma((POWER, CHUNKS, groups - 1)),
        dma((POWER, CHUNKS, groups - 1)),
    ]
    return pl.pallas_call(
        functools.partial(body, cycles, groups),
        out_shape=jax.ShapeDtypeStruct((blk, samples), f32),
        in_specs=[pl.BlockSpec(memory_space=pl.ANY)] * 6,
        out_specs=pl.BlockSpec(memory_space=pltpu.VMEM),
        scratch_shapes=scratch,
        compiler_params=pltpu.CompilerParams(collective_id=0, has_side_effects=True),
        name="power_steps",
    )(
        interior_factor[0],
        interface_coupling[0],
        interface_block[0],
        sample_panel,
        index_map,
        block_count,
    )


def solution(mesh):
    return jax.shard_map(
        local,
        mesh=mesh,
        in_specs=(
            P(("sub", "grp"), None, None),
            P(("sub", "grp"), None, None),
            P(("sub", "grp"), None, None),
            P("sub", None),
            P(("sub", "grp"), None),
            P(("sub", "grp")),
        ),
        out_specs=P(("sub", "grp"), None),
        check_vma=False,
    )
```
